32 devices in a mesh: lat: 16 (over z, y, x), head: 2 (over core).
Axes of the slice: x: 2, y: 2, z: 4, core: 2. Of those that a mesh axis runs over, the one named last changes fastest.
Arguments:
- grid_latent: bfloat16 [131072, 512], P('lat'), may hold values from -6 to 6
- mesh_latent: bfloat16 [10240, 512], P('lat'), may hold values from -6 to 6
- neighbours: int32 [10240, 16], P('lat'), may hold values from -1 to 131071, as said below
- edge_bias: bfloat16 [10240, 64], P('lat', 'head'), may hold values from -8 to 384
- query_weight: bfloat16 [512, 512], P(None, 'head'), may hold values from -0.25 to 0.25
- key_weight: bfloat16 [512, 512], P(None, 'head'), may hold values from -0.25 to 0.25
- value_weight: bfloat16 [512, 512], P(None, 'head'), may hold values from -0.25 to 0.25
- out_weight: bfloat16 [512, 512], P('head'), may hold values from -0.25 to 0.25
- norm_gain: bfloat16 [512], P('head'), may hold values from 0.5 to 1.5
Outputs:
- mesh_out: bfloat16 [10240, 512], P('lat', 'head')
The draws below stay inside these ranges and needn't reach their ends.
Inputs may be any that keep to these rules, and one draw needn't show every extreme that they name: `neighbours`: every neighbour of mesh node m is -1 or lies in [b * 8192 - 2048, (b + 1) * 8192 + 2048) with b = m // 640; both ends of that range (cut to the grid) are named in every draw; slots 0 and 1 are never -1.
All inputs are finite; a program needn't handle non-finite values.
Results may differ from the reference program's by a relative error of at most 0.0075.
Values may be sent and summed in bfloat16 or wider, within the bound.
No kernel may reach another device: no remote copies, remote signals or barrier semaphores. Data moves between devices by JAX's collectives and lax.ppermute only.
A program may use at most 128 MiB of HBM per device.

```python
import math
import jax
import jax.numpy as jnp
from jax import lax

D = 512
HEADS = 4
K = 16
G_DEV = 8192
M_DEV = 640
HEAD_DIM = 128
HALO = 2048
GRID = 131072
MESH = 10240


def draw_neighbours(key, part):
    mesh_ids = jnp.arange(MESH, dtype=jnp.int32)
    owner = mesh_ids // M_DEV
    lowest = jnp.maximum(owner * G_DEV - HALO, 0)
    highest = jnp.minimum((owner + 1) * G_DEV + HALO, GRID)
    key_pick = jax.random.fold_in(key, 11)
    key_pad = jax.random.fold_in(key, 23)
    offsets = jax.random.randint(key_pick, (MESH, K), 0, (highest - lowest)[:, None])
    picked = lowest[:, None] + offsets
    first = (mesh_ids % M_DEV == 0)[:, None]
    slot = jnp.arange(K, dtype=jnp.int32)[None, :]
    picked = jnp.where(first & (slot == 0), lowest[:, None], picked)
    picked = jnp.where(first & (slot == 1), highest[:, None] - 1, picked)
    padded = (jax.random.randint(key_pad, (MESH, K), 0, 4) == 0) & (slot >= 2)
    return jnp.where(padded, -1, picked).astype(jnp.int32)


def draw_edge_bias(key, part):
    base = jnp.clip(jax.random.normal(jax.random.fold_in(key, 37), (MESH, HEADS * K), jnp.float32), -8.0, 8.0)
    return base.astype(jnp.bfloat16)


def shard_levels(key, extent, cuts, smallest, high):
    def one(dim, shards_of):
        steps = jax.random.uniform(jax.random.fold_in(jax.random.fold_in(key, 6), dim), (shards_of,), jnp.float32, smallest / len(cuts), high / len(cuts))
        return jnp.repeat(jnp.exp(steps), extent[dim] // shards_of).reshape((-1,) + (1,) * (len(extent) - dim - 1))

    level = one(*cuts[0])
    for cut in cuts[1:]:
        level = level * one(*cut)
    return level


def gaussian(key, dims, deviation, limit, shards=(), kind=jnp.bfloat16):
    array = jax.random.normal(key, dims, jnp.float32) * deviation
    if len(shards) > 0:
        array = shard_levels(key, dims, shards, -0.22, 0.18) * array
    return jnp.clip(array, min=-limit, max=limit).astype(kind)


def setup_inputs(seed: int = 0) -> dict:
    splits = jax.random.split(jax.random.key(seed), 10)
    grid_latent = gaussian(splits[0], (GRID, D), 1.0, 6.0, ((0, 16),))
    mesh_latent = gaussian(splits[1], (MESH, D), 1.0, 6.0, ((0, 16),))
    neighbours = draw_neighbours(jax.random.fold_in(splits[9], 71), 0)
    edge_bias = draw_edge_bias(jax.random.fold_in(splits[9], 71), 0)
    query_weight = gaussian(splits[4], (D, D), D ** -0.5, 0.25, ((1, 2),))
    key_weight = gaussian(splits[5], (D, D), D ** -0.5, 0.25, ((1, 2),))
    value_weight = gaussian(splits[6], (D, D), D ** -0.5, 0.25, ((1, 2),))
    out_weight = gaussian(splits[7], (D, D), D ** -0.5, 0.25, ((0, 2),))
    norm_gain = jnp.clip(1.0 + 0.1 * jax.random.normal(splits[8], (D,), jnp.float32), 0.5, 1.5).astype(jnp.bfloat16)
    return dict(grid_latent=grid_latent, mesh_latent=mesh_latent, neighbours=neighbours, edge_bias=edge_bias, query_weight=query_weight, key_weight=key_weight, value_weight=value_weight, out_weight=out_weight, norm_gain=norm_gain)


EPSILON = 1e-05

def reference(grid_latent, mesh_latent, neighbours, edge_bias, query_weight, key_weight, value_weight, out_weight, norm_gain):

    def attend_block(blocks):
        mesh_rows, neigh_rows, bias_rows = blocks
        count = mesh_rows.shape[0]
        queries = jnp.dot(mesh_rows, query_weight, preferred_element_type=jnp.float32).astype(jnp.bfloat16)
        valid = neigh_rows >= 0
        safe_index = jnp.where(valid, neigh_rows, 0).astype(jnp.int32)
        fetched = grid_latent[safe_index.reshape(-1)]
        keys = jnp.dot(fetched, key_weight, preferred_element_type=jnp.float32).astype(jnp.bfloat16)
        values = jnp.dot(fetched, value_weight, preferred_element_type=jnp.float32).astype(jnp.bfloat16)
        keys = keys.reshape(count, K, HEADS, HEAD_DIM).astype(jnp.float32)
        values = values.reshape(count, K, HEADS, HEAD_DIM).astype(jnp.float32)
        query_heads = queries.astype(jnp.float32).reshape(count, HEADS, HEAD_DIM)
        scores = jnp.einsum('bhc,bkhc->bhk', query_heads, keys) * HEAD_DIM ** (-0.5)
        scores = scores + bias_rows.astype(jnp.float32).reshape(count, HEADS, K)
        live = valid[:, None, :]
        scores = jnp.where(live, scores, -1e+30)
        top_score = lax.optimization_barrier(jnp.max(scores, axis=2, keepdims=True))
        weights = jnp.where(live, jnp.exp(scores - top_score), 0.0)
        total = lax.optimization_barrier(jnp.sum(weights, axis=2))
        mixed = jnp.einsum('bhk,bkhc->bhc', weights, values) / total[:, :, None]
        attended = mixed.reshape(count, D).astype(jnp.bfloat16)
        projected = jnp.dot(attended, out_weight, preferred_element_type=jnp.float32)
        updated = mesh_rows.astype(jnp.float32) + projected
        mean = lax.optimization_barrier(jnp.sum(updated, axis=1)) / D
        variance = lax.optimization_barrier(jnp.sum(updated * updated, axis=1)) / D - mean * mean
        normed = (updated - mean[:, None]) * lax.rsqrt(variance[:, None] + EPSILON) * norm_gain.astype(jnp.float32)
        return normed.astype(jnp.bfloat16)
    block = math.gcd(MESH, 512)
    nblocks = MESH // block
    result = lax.map(attend_block, (mesh_latent.reshape(nblocks, block, D), neighbours.reshape(nblocks, block, K), edge_bias.reshape(nblocks, block, HEADS * K)))
    return result.reshape(MESH, D)
```

```python
import jax
import jax.numpy as jnp
from jax import lax
from jax.experimental import pallas as pl
from jax.experimental.pallas import tpu as pltpu
from jax.sharding import PartitionSpec as P

K = 16
HEAD_DIM = 128
HALO = 2048
LANES = 128
NODES = 64
STAGE = 1024

EPSILON = 1e-05


def attend_kernel(
    rows_ref, head_ref,
    band_ref, low_ref, low_peer_ref, high_ref, high_peer_ref,
    mesh_ref, bias_ref, gain_ref, weights_ref, peer_weights_ref,
    out_ref,
    source_ref, stage_ref, picked_ref, queries_ref, kv_ref, score_ref, mixed_ref, sems,
):
    width = mesh_ref.shape[1]
    half = width // 2
    chunks = width // LANES
    nodes = mesh_ref.shape[0]
    slots = NODES * K
    head = head_ref[0]
    band = band_ref.shape[0]

    pieces = [(band_ref, p * STAGE, HALO + p * STAGE) for p in range(band // STAGE)]
    for mine, peer, base in ((low_ref, low_peer_ref, 0), (high_ref, high_peer_ref, HALO + band)):
        part = mine.shape[0]
        for p in range(part // STAGE):
            pieces.append((mine, p * STAGE, base + head * part + p * STAGE))
            pieces.append((peer, p * STAGE, base + (1 - head) * part + p * STAGE))

    def copy(n):
        ref, start, _ = pieces[n]
        return pltpu.make_async_copy(
            ref.at[pl.ds(start, STAGE), :], stage_ref.at[n % 2], sems.at[n % 2]
        )

    copy(0).start()
    for n in range(len(pieces)):
        if n + 1 < len(pieces):
            copy(n + 1).start()
        copy(n).wait()
        target = pieces[n][2]

        def convert(step, _, n=n, target=target):
            rows = 64
            block = stage_ref[n % 2, pl.ds(pl.multiple_of(step * rows, rows), rows), :]
            block = block.astype(jnp.float32)
            start = pl.multiple_of((target + step * rows) * chunks, rows * chunks)
            for c in range(chunks):
                source_ref[pl.ds(start + c, rows, stride=chunks), :] = block[
                    :, c * LANES : (c + 1) * LANES
                ]
            return 0

        lax.fori_loop(0, STAGE // 64, convert, 0)

    def weight(ref, n):
        return ref[pl.ds(n * width, width), :]

    for part, ref in enumerate((weights_ref, peer_weights_ref)):
        q = jnp.dot(mesh_ref[...], weight(ref, 0), preferred_element_type=jnp.float32)
        queries_ref[:, part * half : (part + 1) * half] = q.astype(jnp.bfloat16).astype(
            jnp.float32
        ) * HEAD_DIM ** (-0.5)

    lane = lax.broadcasted_iota(jnp.int32, (half, half), 0) // HEAD_DIM
    same = (lane == lax.broadcasted_iota(jnp.int32, (half, half), 1) // HEAD_DIM)
    ones = jnp.where(same, 1.0, 0.0).astype(jnp.bfloat16)

    def block_step(b, _):
        def pick(step, _):
            unroll = 32
            base = b * slots + step * unroll
            to = pl.multiple_of(step * unroll * chunks, unroll * chunks)
            for u in range(unroll):
                row = pl.multiple_of(rows_ref[base + u], chunks)
                picked_ref[pl.ds(to + u * chunks, chunks), :] = source_ref[pl.ds(row, chunks), :]
            return 0

        lax.fori_loop(0, slots // 32, pick, 0)
        latents = jnp.concatenate(
            [
                picked_ref[pl.ds(c, slots, stride=chunks), :].astype(jnp.bfloat16)
                for c in range(chunks)
            ],
            axis=1,
        )
        for part, ref in enumerate((weights_ref, peer_weights_ref)):
            for n in range(2):
                r = jnp.dot(latents, weight(ref, 1 + n), preferred_element_type=jnp.float32)
                kv_ref[n, :, part * half : (part + 1) * half] = r.astype(jnp.bfloat16)
        first = pl.multiple_of(b * NODES, NODES)
        q = queries_ref[pl.ds(first, NODES), :]
        for k in range(K):
            product = kv_ref[0, k * NODES : (k + 1) * NODES, :].astype(jnp.float32) * q
            score_ref[k * NODES : (k + 1) * NODES, :] = product
        for part in range(2):
            product = score_ref[:, part * half : (part + 1) * half]
            upper = product.astype(jnp.bfloat16)
            lower = (product - upper.astype(jnp.float32)).astype(jnp.bfloat16)
            score_ref[:, part * half : (part + 1) * half] = jnp.dot(
                upper, ones, preferred_element_type=jnp.float32
            ) + jnp.dot(lower, ones, preferred_element_type=jnp.float32)

        def mix(step, _):
            tile = 16
            at = pl.multiple_of(step * tile, tile)
            for h in range(chunks):
                cols = slice(h * LANES, (h + 1) * LANES)
                scores = []
                for k in range(K):
                    c = h * K + k
                    bias = bias_ref[pl.ds(first + at, tile), c : c + 1]
                    scores.append(
                        score_ref[pl.ds(k * NODES + at, tile), cols]
                        + jnp.broadcast_to(bias, (tile, LANES))
                    )
                top = scores[0]
                for k in range(1, K):
                    top = jnp.maximum(top, scores[k])
                total = jnp.zeros((tile, LANES), jnp.float32)
                summed = jnp.zeros((tile, LANES), jnp.float32)
                for k in range(K):
                    w = jnp.exp(scores[k] - top)
                    total = total + w
                    summed = summed + w * kv_ref[1, pl.ds(k * NODES + at, tile), cols].astype(
                        jnp.float32
                    )
                mixed_ref[pl.ds(first + at, tile), cols] = (summed / total).astype(jnp.bfloat16)
            return 0

        lax.fori_loop(0, NODES // 16, mix, 0)
        return 0

    lax.fori_loop(0, nodes // NODES, block_step, 0)

    for part in range(2):
        cols = slice(part * half, (part + 1) * half)
        projected = jnp.dot(
            mixed_ref[:, :half],
            weights_ref[pl.ds((3 * width + part * half), half), :],
            preferred_element_type=jnp.float32,
        ) + jnp.dot(
            mixed_ref[:, half:],
            peer_weights_ref[pl.ds((3 * width + part * half), half), :],
            preferred_element_type=jnp.float32,
        )
        queries_ref[:, cols] = mesh_ref[:, cols].astype(jnp.float32) + projected
    updated = queries_ref[...]
    mean = jnp.sum(updated, axis=1, keepdims=True) / width
    variance = jnp.sum(updated * updated, axis=1, keepdims=True) / width - mean * mean
    normed = (updated - mean) * lax.rsqrt(variance + EPSILON) * gain_ref[...]
    out_ref[0] = normed[:, :half].astype(jnp.bfloat16)
    out_ref[1] = normed[:, half:].astype(jnp.bfloat16)


def shards(
    grid_latent,
    mesh_latent,
    neighbours,
    edge_bias,
    query_weight,
    key_weight,
    value_weight,
    out_weight,
    norm_gain,
):
    band, width = grid_latent.shape
    count = mesh_latent.shape[0]
    nodes = count // 2
    half = width // 2
    part = HALO // 2
    head = lax.axis_index("head")
    lat_pos = lax.axis_index("lat")
    lats = lax.axis_size("lat")
    forward = [(i, i + 1) for i in range(lats - 1)]
    backward = [(i + 1, i) for i in range(lats - 1)]
    swap = [(0, 1), (1, 0)]

    low = lax.ppermute(
        lax.dynamic_slice_in_dim(grid_latent, band - HALO + head * part, part, 0), "lat", forward
    )
    high = lax.ppermute(
        lax.dynamic_slice_in_dim(grid_latent, head * part, part, 0), "lat", backward
    )

    packed = jnp.concatenate(
        [query_weight, key_weight, value_weight, out_weight[:, :half], out_weight[:, half:]], axis=0
    )
    peer_packed = lax.ppermute(packed, "head", swap)
    theirs = lax.dynamic_slice_in_dim(edge_bias, (1 - head) * nodes, nodes, 0)
    mine = lax.dynamic_slice_in_dim(edge_bias, head * nodes, nodes, 0)
    peer_bias = lax.ppermute(theirs, "head", swap)
    peer_gain = lax.ppermute(norm_gain, "head", swap)
    gain = jnp.where(
        head == 0,
        jnp.concatenate([norm_gain, peer_gain]),
        jnp.concatenate([peer_gain, norm_gain]),
    ).astype(jnp.float32)[None, :]

    my_mesh = lax.dynamic_slice_in_dim(mesh_latent, head * nodes, nodes, 0)
    my_neighbours = lax.dynamic_slice_in_dim(neighbours, head * nodes, nodes, 0)
    valid = my_neighbours >= 0
    bias = jnp.where(
        jnp.tile(valid, (1, width // HEAD_DIM)),
        jnp.concatenate([mine, peer_bias], axis=1).astype(jnp.float32),
        -1e30,
    )
    rows = jnp.where(valid, my_neighbours - (lat_pos * band - HALO), HALO) * (width // LANES)
    rows = rows.reshape(nodes // NODES, NODES, K).transpose(0, 2, 1).reshape(-1)

    low_peer = lax.ppermute(low, "head", swap)
    high_peer = lax.ppermute(high, "head", swap)

    smem = pl.BlockSpec(memory_space=pltpu.SMEM)
    anywhere = pl.BlockSpec(memory_space=pl.ANY)
    vmem = pl.BlockSpec(memory_space=pltpu.VMEM)
    slots = NODES * K
    halves = pl.pallas_call(
        attend_kernel,
        out_shape=jax.ShapeDtypeStruct((2, nodes, half), jnp.bfloat16),
        in_specs=[smem, smem] + [anywhere] * 5 + [vmem] * 5,
        out_specs=vmem,
        scratch_shapes=[
            pltpu.VMEM(((band + 2 * HALO) * (width // LANES), LANES), jnp.float32),
            pltpu.VMEM((2, STAGE, width), jnp.bfloat16),
            pltpu.VMEM((slots * (width // LANES), LANES), jnp.float32),
            pltpu.VMEM((nodes, width), jnp.float32),
            pltpu.VMEM((2, slots, width), jnp.bfloat16),
            pltpu.VMEM((slots, width), jnp.float32),
            pltpu.VMEM((nodes, width), jnp.bfloat16),
            pltpu.SemaphoreType.DMA((2,)),
        ],
        compiler_params=pltpu.CompilerParams(vmem_limit_bytes=56 * 1024 * 1024),
        name="attend",
    )(
        rows, head.reshape(1).astype(jnp.int32),
        grid_latent, low, low_peer, high, high_peer,
        my_mesh, bias, gain, packed, peer_packed,
    )
    keep = lax.dynamic_index_in_dim(halves, head, 0, keepdims=False)
    give = lax.dynamic_index_in_dim(halves, 1 - head, 0, keepdims=False)
    got = lax.ppermute(give, "head", swap)
    return jnp.where(
        head == 0, jnp.concatenate([keep, got], axis=0), jnp.concatenate([got, keep], axis=0)
    )


def solution(mesh):
    in_specs = (
        P("lat", None),
        P("lat", None),
        P("lat", None),
        P("lat", "head"),
        P(None, "head"),
        P(None, "head"),
        P(None, "head"),
        P("head", None),
        P("head"),
    )
    out_specs = P("lat", "head")
    return jax.shard_map(shards, mesh=mesh, in_specs=in_specs, out_specs=out_specs, check_vma=False)
```

```python
import jax
import jax.numpy as jnp
from jax import lax
from jax.experimental import pallas as pl
from jax.experimental.pallas import tpu as pltpu
from jax.sharding import PartitionSpec as P


K = 16
HEAD_DIM = 128
HALO = 2048
LANES = 128
NODES = 64
STAGE = 1024
FEW = 4

EPSILON = 1e-05


def stage(pieces, stage_ref, source_ref, sems):
    width = stage_ref.shape[2]
    chunks = width // LANES

    def copy(n):
        ref, start, _ = pieces[n]
        return pltpu.make_async_copy(
            ref.at[pl.ds(start, STAGE), :], stage_ref.at[n % 2], sems.at[n % 2]
        )

    copy(0).start()
    for n in range(len(pieces)):
        if n + 1 < len(pieces):
            copy(n + 1).start()
        copy(n).wait()
        target = pieces[n][2]

        def convert(step, _, n=n, target=target):
            rows = 64
            block = stage_ref[n % 2, pl.ds(pl.multiple_of(step * rows, rows), rows), :]
            block = block.astype(jnp.float32)
            start = pl.multiple_of((target + step * rows) * chunks, rows * chunks)
            for c in range(chunks):
                source_ref[pl.ds(start + c, rows, stride=chunks), :] = block[
                    :, c * LANES : (c + 1) * LANES
                ]
            return 0

        lax.fori_loop(0, STAGE // 64, convert, 0)


def head_sums(half):
    lane = lax.broadcasted_iota(jnp.int32, (half, half), 0) // HEAD_DIM
    same = lane == lax.broadcasted_iota(jnp.int32, (half, half), 1) // HEAD_DIM
    return jnp.where(same, 1.0, 0.0).astype(jnp.bfloat16)


def attend_slots(
    b, begin, taken, fresh, rows_ref, bias_ref, queries_ref, weights, source_ref,
    picked_ref, kv_ref, score_ref, top_ref, total_ref, summed_ref, ones,
):
    width = queries_ref.shape[1]
    half = width // 2
    chunks = width // LANES
    slots = taken * NODES
    unroll = 32

    def pick(step, _):
        base = (b * K + begin) * NODES + step * unroll
        to = pl.multiple_of(step * unroll * chunks, unroll * chunks)
        for u in range(unroll):
            row = pl.multiple_of(rows_ref[base + u], chunks)
            picked_ref[pl.ds(to + u * chunks, chunks), :] = source_ref[pl.ds(row, chunks), :]
        return 0

    lax.fori_loop(0, slots // unroll, pick, 0)
    latents = jnp.concatenate(
        [picked_ref[pl.ds(c, slots, stride=chunks), :].astype(jnp.bfloat16) for c in range(chunks)],
        axis=1,
    )
    for part, ref in enumerate(weights):
        for n in range(2):
            r = jnp.dot(
                latents, ref[pl.ds((1 + n) * width, width), :], preferred_element_type=jnp.float32
            )
            kv_ref[n, :, part * half : (part + 1) * half] = r.astype(jnp.bfloat16)
    first = pl.multiple_of(b * NODES, NODES)
    q = queries_ref[pl.ds(first, NODES), :]
    for k in range(taken):
        near = slice(k * NODES, (k + 1) * NODES)
        score_ref[near, :] = kv_ref[0, near, :].astype(jnp.float32) * q
    for part in range(2):
        cols = slice(part * half, (part + 1) * half)
        product = score_ref[:, cols]
        upper = product.astype(jnp.bfloat16)
        lower = (product - upper.astype(jnp.float32)).astype(jnp.bfloat16)
        score_ref[:, cols] = jnp.dot(upper, ones, preferred_element_type=jnp.float32) + jnp.dot(
            lower, ones, preferred_element_type=jnp.float32
        )

    tile = 16

    def mix(step, _):
        at = pl.multiple_of(step * tile, tile)
        here = pl.ds(first + at, tile)
        for h in range(chunks):
            cols = slice(h * LANES, (h + 1) * LANES)
            scores = []
            for k in range(taken):
                bias = bias_ref[begin // taken, here, h * taken + k : h * taken + k + 1]
                scores.append(
                    score_ref[pl.ds(k * NODES + at, tile), cols]
                    + jnp.broadcast_to(bias, (tile, LANES))
                )
            top = scores[0]
            for score in scores[1:]:
                top = jnp.maximum(top, score)
            if fresh:
                total = jnp.zeros((tile, LANES), jnp.float32)
                summed = jnp.zeros((tile, LANES), jnp.float32)
            else:
                before = top_ref[here, cols]
                top = jnp.maximum(top, before)
                fade = jnp.exp(before - top)
                total = total_ref[here, cols] * fade
                summed = summed_ref[here, cols] * fade
            for k in range(taken):
                w = jnp.exp(scores[k] - top)
                total = total + w
                summed = summed + w * kv_ref[1, pl.ds(k * NODES + at, tile), cols].astype(
                    jnp.float32
                )
            top_ref[here, cols] = top
            total_ref[here, cols] = total
            summed_ref[here, cols] = summed
        return 0

    lax.fori_loop(0, NODES // tile, mix, 0)


def band_kernel(
    rows_ref, band_ref, mesh_ref, bias_ref, weights_ref, peer_weights_ref,
    queries_ref, top_ref, total_ref, summed_ref,
    source_ref, stage_ref, picked_ref, kv_ref, score_ref, sems,
):
    nodes, width = mesh_ref.shape
    half = width // 2
    weights = (weights_ref, peer_weights_ref)
    pieces = [(band_ref, p * STAGE, p * STAGE) for p in range(band_ref.shape[0] // STAGE)]
    stage(pieces, stage_ref, source_ref, sems)
    for part, ref in enumerate(weights):
        q = jnp.dot(mesh_ref[...], ref[pl.ds(0, width), :], preferred_element_type=jnp.float32)
        queries_ref[:, part * half : (part + 1) * half] = q.astype(jnp.bfloat16).astype(
            jnp.float32
        ) * HEAD_DIM ** (-0.5)
    ones = head_sums(half)

    def block_step(b, _):
        attend_slots(
            b, 0, K, True, rows_ref, bias_ref, queries_ref, weights, source_ref,
            picked_ref, kv_ref, score_ref, top_ref, total_ref, summed_ref, ones,
        )
        return 0

    lax.fori_loop(0, nodes // NODES, block_step, 0)


def halo_kernel(
    rows_ref, trips_ref, head_ref, low_ref, low_peer_ref, high_ref, high_peer_ref,
    mesh_ref, bias_ref, gain_ref, weights_ref, peer_weights_ref,
    queries_ref, top_in_ref, total_in_ref, summed_in_ref,
    keep_ref, give_ref,
    source_ref, stage_ref, picked_ref, kv_ref, score_ref, top_ref, total_ref, summed_ref,
    mixed_ref, sems,
):
    nodes, width = mesh_ref.shape
    half = width // 2
    head = head_ref[0]
    weights = (weights_ref, peer_weights_ref)
    pieces = []
    for mine, peer, base in ((low_ref, low_peer_ref, 0), (high_ref, high_peer_ref, HALO)):
        part = mine.shape[0]
        for p in range(part // STAGE):
            pieces.append((mine, p * STAGE, base + head * part + p * STAGE))
            pieces.append((peer, p * STAGE, base + (1 - head) * part + p * STAGE))
    stage(pieces, stage_ref, source_ref, sems)
    top_ref[...] = top_in_ref[...]
    total_ref[...] = total_in_ref[...]
    summed_ref[...] = summed_in_ref[...]
    ones = head_sums(half)

    def block_step(b, _):
        def trip(t, _):
            attend_slots(
                b, t * FEW, FEW, False, rows_ref, bias_ref, queries_ref, weights, source_ref,
                picked_ref, kv_ref, score_ref, top_ref, total_ref, summed_ref, ones,
            )
            return 0

        lax.fori_loop(0, trips_ref[b], trip, 0)
        return 0

    lax.fori_loop(0, nodes // NODES, block_step, 0)

    mixed_ref[...] = (summed_ref[...] / total_ref[...]).astype(jnp.bfloat16)
    for part in range(2):
        cols = slice(part * half, (part + 1) * half)
        out_rows = pl.ds(3 * width + part * half, half)
        projected = jnp.dot(
            mixed_ref[:, :half], weights_ref[out_rows, :], preferred_element_type=jnp.float32
        ) + jnp.dot(
            mixed_ref[:, half:], peer_weights_ref[out_rows, :], preferred_element_type=jnp.float32
        )
        summed_ref[:, cols] = mesh_ref[:, cols].astype(jnp.float32) + projected
    updated = summed_ref[...]
    mean = jnp.sum(updated, axis=1, keepdims=True) / width
    variance = jnp.sum(updated * updated, axis=1, keepdims=True) / width - mean * mean
    normed = (updated - mean) * lax.rsqrt(variance + EPSILON) * gain_ref[...]
    left = normed[:, :half].astype(jnp.bfloat16)
    right = normed[:, half:].astype(jnp.bfloat16)

    @pl.when(head == 0)
    def _():
        keep_ref[...] = left
        give_ref[...] = right

    @pl.when(head != 0)
    def _():
        keep_ref[...] = right
        give_ref[...] = left


def attend(
    grid_latent,
    mesh_latent,
    neighbours,
    edge_bias,
    query_weight,
    key_weight,
    value_weight,
    out_weight,
    norm_gain,
):
    band, width = grid_latent.shape
    count = mesh_latent.shape[0]
    nodes = count // 2
    half = width // 2
    part = HALO // 2
    head = lax.axis_index("head")
    lat_pos = lax.axis_index("lat")
    lats = lax.axis_size("lat")
    forward = [(i, i + 1) for i in range(lats - 1)]
    backward = [(i + 1, i) for i in range(lats - 1)]
    swap = [(0, 1), (1, 0)]

    low = lax.dynamic_slice_in_dim(grid_latent, band - HALO + head * part, part, 0)
    high = lax.dynamic_slice_in_dim(grid_latent, head * part, part, 0)
    low = lax.ppermute(low, "lat", forward)
    high = lax.ppermute(high, "lat", backward)

    packed = jnp.concatenate(
        [query_weight, key_weight, value_weight, out_weight[:, :half], out_weight[:, half:]],
        axis=0,
    )
    peer_packed = lax.ppermute(packed, "head", swap)
    theirs = lax.dynamic_slice_in_dim(edge_bias, (1 - head) * nodes, nodes, 0)
    mine = lax.dynamic_slice_in_dim(edge_bias, head * nodes, nodes, 0)
    peer_bias = lax.ppermute(theirs, "head", swap)
    peer_gain = lax.ppermute(norm_gain, "head", swap)
    gain = jnp.where(
        head == 0,
        jnp.concatenate([norm_gain, peer_gain]),
        jnp.concatenate([peer_gain, norm_gain]),
    ).astype(jnp.float32)[None, :]

    my_mesh = lax.dynamic_slice_in_dim(mesh_latent, head * nodes, nodes, 0)
    my_neighbours = lax.dynamic_slice_in_dim(neighbours, head * nodes, nodes, 0)
    heads = width // HEAD_DIM
    chunks = width // LANES
    blocks = nodes // NODES
    bias = jnp.concatenate([mine, peer_bias], axis=1).astype(jnp.float32)
    slot_neighbours = my_neighbours.T
    place = slot_neighbours - lat_pos * band
    valid = slot_neighbours >= 0
    inside = valid & (place >= 0) & (place < band)
    outside = valid & ~inside

    def order(rows):
        return (rows * chunks).reshape(K, blocks, NODES).transpose(1, 0, 2).reshape(-1)

    band_rows = order(jnp.where(inside, place, 0))
    band_bias = jnp.where(jnp.tile(inside.T, (1, heads)), bias, -1e30)[None]

    halo_place = jnp.where(place < 0, place + HALO, place - band + HALO)
    slot = jnp.arange(K, dtype=jnp.int32)
    earlier = (slot[:, None] < slot[None, :])[:, :, None]
    rank = jnp.sum(jnp.where(earlier & outside[:, None, :], 1, 0), axis=0)
    found = jnp.sum(outside.astype(jnp.int32), axis=0)
    chosen = outside[:, None, :] & (rank[:, None, :] == slot[None, :, None])
    halo_rows = order(jnp.sum(jnp.where(chosen, halo_place[:, None, :], 0), axis=0))
    slot_bias = bias.T.reshape(heads, K, nodes)
    halo_bias = jnp.sum(jnp.where(chosen[None], slot_bias[:, :, None, :], 0.0), axis=1)
    halo_bias = jnp.where(slot[None, :, None] < found[None, None, :], halo_bias, -1e30)
    halo_bias = halo_bias.reshape(heads, K // FEW, FEW, nodes)
    halo_bias = halo_bias.transpose(1, 3, 0, 2).reshape(K // FEW, nodes, heads * FEW)
    trips = (jnp.max(found.reshape(blocks, NODES), axis=1) + (FEW - 1)) // FEW

    smem = pl.BlockSpec(memory_space=pltpu.SMEM)
    anywhere = pl.BlockSpec(memory_space=pl.ANY)
    vmem = pl.BlockSpec(memory_space=pltpu.VMEM)
    params = pltpu.CompilerParams(vmem_limit_bytes=48 * 1024 * 1024)
    state = jax.ShapeDtypeStruct((nodes, width), jnp.float32)

    def scratch(held, slots):
        return [
            pltpu.VMEM((held * chunks, LANES), jnp.float32),
            pltpu.VMEM((2, STAGE, width), jnp.bfloat16),
            pltpu.VMEM((slots * chunks, LANES), jnp.float32),
            pltpu.VMEM((2, slots, width), jnp.bfloat16),
            pltpu.VMEM((slots, width), jnp.float32),
        ]

    my_mesh, gain, trips, halo_rows, halo_bias = lax.optimization_barrier(
        (my_mesh, gain, trips, halo_rows, halo_bias)
    )
    partial = pl.pallas_call(
        band_kernel,
        out_shape=[state] * 4,
        in_specs=[smem, anywhere] + [vmem] * 4,
        out_specs=[vmem] * 4,
        scratch_shapes=scratch(band, NODES * K) + [pltpu.SemaphoreType.DMA((2,))],
        compiler_params=params,
        name="band",
    )(band_rows, grid_latent, my_mesh, band_bias, packed, peer_packed)

    low_peer = lax.ppermute(low, "head", swap)
    high_peer = lax.ppermute(high, "head", swap)
    out = jax.ShapeDtypeStruct((nodes, half), jnp.bfloat16)
    keep, give = pl.pallas_call(
        halo_kernel,
        out_shape=[out, out],
        in_specs=[smem] * 3 + [anywhere] * 4 + [vmem] * 9,
        out_specs=[vmem, vmem],
        scratch_shapes=scratch(2 * HALO, NODES * FEW)
        + [pltpu.VMEM((nodes, width), jnp.float32)] * 3
        + [pltpu.VMEM((nodes, width), jnp.bfloat16), pltpu.SemaphoreType.DMA((2,))],
        compiler_params=params,
        name="halo",
    )(
        halo_rows, trips, head.reshape(1).astype(jnp.int32), low, low_peer, high, high_peer,
        my_mesh, halo_bias, gain, packed, peer_packed, *partial,
    )
    got = lax.ppermute(give, "head", swap)
    return jnp.where(
        head == 0, jnp.concatenate([keep, got], axis=0), jnp.concatenate([got, keep], axis=0)
    )


def solution(mesh):
    in_specs = (
        P("lat", None),
        P("lat", None),
        P("lat", None),
        P("lat", "head"),
        P(None, "head"),
        P(None, "head"),
        P(None, "head"),
        P("head", None),
        P("head"),
    )
    out_specs = P("lat", "head")
    return jax.shard_map(attend, mesh=mesh, in_specs=in_specs, out_specs=out_specs, check_vma=False)
```

```python
import jax
import jax.numpy as jnp
from jax import lax
from jax.experimental import pallas as pl
from jax.experimental.pallas import tpu as pltpu
from jax.sharding import PartitionSpec as P


K = 16
HEAD_DIM = 128
HALO = 2048
LANES = 128
NODES = 64
STAGE = 1024
FEW = 4

EPSILON = 1e-05


def stage(pieces, stage_ref, source_ref, sems):
    width = stage_ref.shape[2]
    chunks = width // LANES

    def copy(n):
        ref, start, _ = pieces[n]
        return pltpu.make_async_copy(
            ref.at[pl.ds(start, STAGE), :], stage_ref.at[n % 2], sems.at[n % 2]
        )

    copy(0).start()
    for n in range(len(pieces)):
        if n + 1 < len(pieces):
            copy(n + 1).start()
        copy(n).wait()
        target = pieces[n][2]

        def convert(step, _, n=n, target=target):
            rows = 64
            block = stage_ref[n % 2, pl.ds(pl.multiple_of(step * rows, rows), rows), :]
            block = block.astype(jnp.float32)
            start = pl.multiple_of((target + step * rows) * chunks, rows * chunks)
            for c in range(chunks):
                source_ref[pl.ds(start + c, rows, stride=chunks), :] = block[
                    :, c * LANES : (c + 1) * LANES
                ]
            return 0

        lax.fori_loop(0, STAGE // 64, convert, 0)


def head_sums(half):
    lane = lax.broadcasted_iota(jnp.int32, (half, half), 0) // HEAD_DIM
    same = lane == lax.broadcasted_iota(jnp.int32, (half, half), 1) // HEAD_DIM
    return jnp.where(same, 1.0, 0.0).astype(jnp.bfloat16)


def attend_slots(
    b, begin, taken, fresh, rows_ref, bias_ref, queries_ref, weights, source_ref,
    picked_ref, kv_ref, score_ref, top_ref, total_ref, summed_ref, ones,
):
    width = queries_ref.shape[1]
    half = width // 2
    chunks = width // LANES
    slots = taken * NODES
    unroll = 32

    def pick(step, _):
        base = (b * K + begin) * NODES + step * unroll
        to = pl.multiple_of(step * unroll * chunks, unroll * chunks)
        for u in range(unroll):
            row = pl.multiple_of(rows_ref[base + u], chunks)
            picked_ref[pl.ds(to + u * chunks, chunks), :] = source_ref[pl.ds(row, chunks), :]
        return 0

    lax.fori_loop(0, slots // unroll, pick, 0)
    latents = jnp.concatenate(
        [picked_ref[pl.ds(c, slots, stride=chunks), :].astype(jnp.bfloat16) for c in range(chunks)],
        axis=1,
    )
    for part, ref in enumerate(weights):
        for n in range(2):
            r = jnp.dot(
                latents, ref[pl.ds((1 + n) * width, width), :], preferred_element_type=jnp.float32
            )
            kv_ref[n, :, part * half : (part + 1) * half] = r.astype(jnp.bfloat16)
    first = pl.multiple_of(b * NODES, NODES)
    q = queries_ref[pl.ds(first, NODES), :]
    for k in range(taken):
        near = slice(k * NODES, (k + 1) * NODES)
        score_ref[near, :] = kv_ref[0, near, :].astype(jnp.float32) * q
    for part in range(2):
        cols = slice(part * half, (part + 1) * half)
        product = score_ref[:, cols]
        upper = product.astype(jnp.bfloat16)
        lower = (product - upper.astype(jnp.float32)).astype(jnp.bfloat16)
        score_ref[:, cols] = jnp.dot(upper, ones, preferred_element_type=jnp.float32) + jnp.dot(
            lower, ones, preferred_element_type=jnp.float32
        )

    tile = 16

    def mix(step, _):
        at = pl.multiple_of(step * tile, tile)
        here = pl.ds(first + at, tile)
        for h in range(chunks):
            cols = slice(h * LANES, (h + 1) * LANES)
            scores = []
            for k in range(taken):
                bias = bias_ref[begin // taken, here, h * taken + k : h * taken + k + 1]
                scores.append(
                    score_ref[pl.ds(k * NODES + at, tile), cols]
                    + jnp.broadcast_to(bias, (tile, LANES))
                )
            top = scores[0]
            for score in scores[1:]:
                top = jnp.maximum(top, score)
            if fresh:
                total = jnp.zeros((tile, LANES), jnp.float32)
                summed = jnp.zeros((tile, LANES), jnp.float32)
            else:
                before = top_ref[here, cols]
                top = jnp.maximum(top, before)
                fade = jnp.exp(before - top)
                total = total_ref[here, cols] * fade
                summed = summed_ref[here, cols] * fade
            for k in range(taken):
                w = jnp.exp(scores[k] - top)
                total = total + w
                summed = summed + w * kv_ref[1, pl.ds(k * NODES + at, tile), cols].astype(
                    jnp.float32
                )
            top_ref[here, cols] = top
            total_ref[here, cols] = total
            summed_ref[here, cols] = summed
        return 0

    lax.fori_loop(0, NODES // tile, mix, 0)


def band_kernel(
    rows_ref, band_ref, mesh_ref, bias_ref, weights_ref, peer_weights_ref,
    queries_out_ref, top_out_ref, total_out_ref, summed_out_ref,
    source_ref, stage_ref, picked_ref, kv_ref, score_ref,
    queries_ref, top_ref, total_ref, summed_ref, sems, state_sems,
):
    nodes, width = mesh_ref.shape
    half = width // 2
    weights = (weights_ref, peer_weights_ref)
    pieces = [(band_ref, p * STAGE, p * STAGE) for p in range(band_ref.shape[0] // STAGE)]
    stage(pieces, stage_ref, source_ref, sems)
    for part, ref in enumerate(weights):
        q = jnp.dot(mesh_ref[...], ref[pl.ds(0, width), :], preferred_element_type=jnp.float32)
        queries_ref[:, part * half : (part + 1) * half] = q.astype(jnp.bfloat16).astype(
            jnp.float32
        ) * HEAD_DIM ** (-0.5)
    ones = head_sums(half)

    def block_step(b, _):
        attend_slots(
            b, 0, K, True, rows_ref, bias_ref, queries_ref, weights, source_ref,
            picked_ref, kv_ref, score_ref, top_ref, total_ref, summed_ref, ones,
        )
        return 0

    lax.fori_loop(0, nodes // NODES, block_step, 0)
    copies = [
        pltpu.make_async_copy(held, out, state_sems.at[n])
        for n, (held, out) in enumerate(
            (
                (queries_ref, queries_out_ref),
                (top_ref, top_out_ref),
                (total_ref, total_out_ref),
                (summed_ref, summed_out_ref),
            )
        )
    ]
    for copy in copies:
        copy.start()
    for copy in copies:
        copy.wait()


def halo_kernel(
    rows_ref, trips_ref, head_ref, low_ref, low_peer_ref, high_ref, high_peer_ref,
    mesh_ref, bias_ref, gain_ref, unsort_ref, weights_ref, peer_weights_ref,
    queries_in_ref, top_in_ref, total_in_ref, summed_in_ref,
    keep_ref, give_ref,
    source_ref, stage_ref, picked_ref, kv_ref, score_ref,
    queries_ref, top_ref, total_ref, summed_ref, sems, state_sems, mixed_ref,
):
    nodes, width = mesh_ref.shape
    half = width // 2
    head = head_ref[0]
    weights = (weights_ref, peer_weights_ref)
    pieces = []
    for mine, peer, base in ((low_ref, low_peer_ref, 0), (high_ref, high_peer_ref, HALO)):
        part = mine.shape[0]
        for p in range(part // STAGE):
            pieces.append((mine, p * STAGE, base + head * part + p * STAGE))
            pieces.append((peer, p * STAGE, base + (1 - head) * part + p * STAGE))
    copies = [
        pltpu.make_async_copy(given, held, state_sems.at[n])
        for n, (given, held) in enumerate(
            (
                (queries_in_ref, queries_ref),
                (top_in_ref, top_ref),
                (total_in_ref, total_ref),
                (summed_in_ref, summed_ref),
            )
        )
    ]
    for copy in copies:
        copy.start()
    stage(pieces, stage_ref, source_ref, sems)
    for copy in copies:
        copy.wait()
    ones = head_sums(half)

    def block_step(b, _):
        def trip(t, _):
            attend_slots(
                b, t * FEW, FEW, False, rows_ref, bias_ref, queries_ref, weights, source_ref,
                picked_ref, kv_ref, score_ref, top_ref, total_ref, summed_ref, ones,
            )
            return 0

        lax.fori_loop(0, trips_ref[b], trip, 0)
        return 0

    lax.fori_loop(0, nodes // NODES, block_step, 0)

    mixed_ref[...] = (summed_ref[...] / total_ref[...]).astype(jnp.bfloat16)
    for part in range(2):
        cols = slice(part * half, (part + 1) * half)
        out_rows = pl.ds(3 * width + part * half, half)
        projected = jnp.dot(
            mixed_ref[:, :half], weights_ref[out_rows, :], preferred_element_type=jnp.float32
        ) + jnp.dot(
            mixed_ref[:, half:], peer_weights_ref[out_rows, :], preferred_element_type=jnp.float32
        )
        summed_ref[:, cols] = mesh_ref[:, cols].astype(jnp.float32) + projected
    updated = summed_ref[...]
    mean = jnp.sum(updated, axis=1, keepdims=True) / width
    variance = jnp.sum(updated * updated, axis=1, keepdims=True) / width - mean * mean
    normed = (updated - mean) * lax.rsqrt(variance + EPSILON) * gain_ref[...]
    normed = jnp.dot(
        unsort_ref[...], normed.astype(jnp.bfloat16), preferred_element_type=jnp.float32
    ).astype(jnp.bfloat16)
    left = normed[:, :half]
    right = normed[:, half:]

    @pl.when(head == 0)
    def _():
        keep_ref[...] = left
        give_ref[...] = right

    @pl.when(head != 0)
    def _():
        keep_ref[...] = right
        give_ref[...] = left


def attend(
    grid_latent,
    mesh_latent,
    neighbours,
    edge_bias,
    query_weight,
    key_weight,
    value_weight,
    out_weight,
    norm_gain,
):
    band, width = grid_latent.shape
    count = mesh_latent.shape[0]
    nodes = count // 2
    half = width // 2
    part = HALO // 2
    head = lax.axis_index("head")
    lat_pos = lax.axis_index("lat")
    lats = lax.axis_size("lat")
    forward = [(i, i + 1) for i in range(lats - 1)]
    backward = [(i + 1, i) for i in range(lats - 1)]
    swap = [(0, 1), (1, 0)]

    low = lax.dynamic_slice_in_dim(grid_latent, band - HALO + head * part, part, 0)
    high = lax.dynamic_slice_in_dim(grid_latent, head * part, part, 0)
    low = lax.ppermute(low, "lat", forward)
    high = lax.ppermute(high, "lat", backward)

    packed = jnp.concatenate(
        [query_weight, key_weight, value_weight, out_weight[:, :half], out_weight[:, half:]],
        axis=0,
    )
    peer_packed = lax.ppermute(packed, "head", swap)
    theirs = lax.dynamic_slice_in_dim(edge_bias, (1 - head) * nodes, nodes, 0)
    mine = lax.dynamic_slice_in_dim(edge_bias, head * nodes, nodes, 0)
    peer_bias = lax.ppermute(theirs, "head", swap)
    peer_gain = lax.ppermute(norm_gain, "head", swap)
    gain = jnp.where(
        head == 0,
        jnp.concatenate([norm_gain, peer_gain]),
        jnp.concatenate([peer_gain, norm_gain]),
    ).astype(jnp.float32)[None, :]

    my_mesh = lax.dynamic_slice_in_dim(mesh_latent, head * nodes, nodes, 0)
    my_neighbours = lax.dynamic_slice_in_dim(neighbours, head * nodes, nodes, 0)
    heads = width // HEAD_DIM
    chunks = width // LANES
    blocks = nodes // NODES
    place = my_neighbours - lat_pos * band
    leaves = (my_neighbours >= 0) & ((place < 0) | (place >= band))
    number = jnp.arange(nodes, dtype=jnp.int32)
    weight = jnp.sum(leaves.astype(jnp.int32), axis=1) * nodes + (nodes - 1 - number)
    before = jnp.sum((weight[:, None] > weight[None, :]).astype(jnp.int32), axis=0)
    sort = (before[None, :] == number[:, None]).astype(jnp.bfloat16)
    unsort = (before[:, None] == number[None, :]).astype(jnp.bfloat16)
    raised = my_neighbours + 1
    digits = [(raised >> shift) & 255 for shift in (0, 8, 16)]
    mixed = jnp.concatenate(
        [my_mesh, mine, peer_bias] + [digit.astype(jnp.bfloat16) for digit in digits], axis=1
    )
    mixed = jnp.dot(sort, mixed, preferred_element_type=jnp.float32)
    my_mesh = mixed[:, :width].astype(jnp.bfloat16)
    bias = mixed[:, width : width + heads * K]
    digits = mixed[:, width + heads * K :].astype(jnp.int32).reshape(nodes, 3, K)
    slot_neighbours = (digits[:, 0] + (digits[:, 1] << 8) + (digits[:, 2] << 16) - 1).T
    place = slot_neighbours - lat_pos * band
    valid = slot_neighbours >= 0
    inside = valid & (place >= 0) & (place < band)
    outside = valid & ~inside

    def order(rows):
        return (rows * chunks).reshape(K, blocks, NODES).transpose(1, 0, 2).reshape(-1)

    band_rows = order(jnp.where(inside, place, 0))
    band_bias = jnp.where(jnp.tile(inside.T, (1, heads)), bias, -1e30)[None]

    halo_place = jnp.where(place < 0, place + HALO, place - band + HALO)
    slot = jnp.arange(K, dtype=jnp.int32)
    earlier = (slot[:, None] < slot[None, :])[:, :, None]
    rank = jnp.sum(jnp.where(earlier & outside[:, None, :], 1, 0), axis=0)
    found = jnp.sum(outside.astype(jnp.int32), axis=0)
    chosen = outside[:, None, :] & (rank[:, None, :] == slot[None, :, None])
    halo_rows = order(jnp.sum(jnp.where(chosen, halo_place[:, None, :], 0), axis=0))
    slot_bias = bias.T.reshape(heads, K, nodes)
    halo_bias = jnp.sum(jnp.where(chosen[None], slot_bias[:, :, None, :], 0.0), axis=1)
    halo_bias = jnp.where(slot[None, :, None] < found[None, None, :], halo_bias, -1e30)
    halo_bias = halo_bias.reshape(heads, K // FEW, FEW, nodes)
    halo_bias = halo_bias.transpose(1, 3, 0, 2).reshape(K // FEW, nodes, heads * FEW)
    trips = (jnp.max(found.reshape(blocks, NODES), axis=1) + (FEW - 1)) // FEW

    smem = pl.BlockSpec(memory_space=pltpu.SMEM)
    anywhere = pl.BlockSpec(memory_space=pltpu.MemorySpace.HBM)
    vmem = pl.BlockSpec(memory_space=pltpu.VMEM)
    state = pltpu.HBM((nodes, width), jnp.float32)

    def params(mib):
        return pltpu.CompilerParams(vmem_limit_bytes=mib * 1024 * 1024)

    def scratch(held, slots):
        return [
            pltpu.VMEM((held * chunks, LANES), jnp.float32),
            pltpu.VMEM((2, STAGE, width), jnp.bfloat16),
            pltpu.VMEM((slots * chunks, LANES), jnp.float32),
            pltpu.VMEM((2, slots, width), jnp.bfloat16),
            pltpu.VMEM((slots, width), jnp.float32),
        ] + [pltpu.VMEM((nodes, width), jnp.float32)] * 4 + [
            pltpu.SemaphoreType.DMA((2,)),
            pltpu.SemaphoreType.DMA((4,)),
        ]

    my_mesh, gain, trips, halo_rows, halo_bias, unsort = lax.optimization_barrier(
        (my_mesh, gain, trips, halo_rows, halo_bias, unsort)
    )
    held_latent = pltpu.with_memory_space_constraint(grid_latent, pltpu.MemorySpace.HBM)
    partial = pl.pallas_call(
        band_kernel,
        out_shape=[state] * 4,
        in_specs=[smem, anywhere] + [vmem] * 4,
        out_specs=[anywhere] * 4,
        scratch_shapes=scratch(band, NODES * K),
        compiler_params=params(40),
        name="band",
    )(band_rows, held_latent, my_mesh, band_bias, packed, peer_packed)

    low_peer = lax.ppermute(low, "head", swap)
    high_peer = lax.ppermute(high, "head", swap)
    low, low_peer, high, high_peer, *partial = [
        pltpu.with_memory_space_constraint(array, pltpu.MemorySpace.HBM)
        for array in (low, low_peer, high, high_peer, *partial)
    ]
    out = jax.ShapeDtypeStruct((nodes, half), jnp.bfloat16)
    keep, give = pl.pallas_call(
        halo_kernel,
        out_shape=[out, out],
        in_specs=[smem] * 3 + [anywhere] * 4 + [vmem] * 6 + [anywhere] * 4,
        out_specs=[vmem, vmem],
        scratch_shapes=scratch(2 * HALO, NODES * FEW) + [pltpu.VMEM((nodes, width), jnp.bfloat16)],
        compiler_params=params(40),
        name="halo",
    )(
        halo_rows, trips, head.reshape(1).astype(jnp.int32), low, low_peer, high, high_peer,
        my_mesh, halo_bias, gain, unsort, packed, peer_packed, *partial,
    )
    got = lax.ppermute(give, "head", swap)
    return jnp.where(
        head == 0, jnp.concatenate([keep, got], axis=0), jnp.concatenate([got, keep], axis=0)
    )


def solution(mesh):
    in_specs = (
        P("lat", None),
        P("lat", None),
        P("lat", None),
        P("lat", "head"),
        P(None, "head"),
        P(None, "head"),
        P(None, "head"),
        P("head", None),
        P("head"),
    )
    out_specs = P("lat", "head")
    return jax.shard_map(attend, mesh=mesh, in_specs=in_specs, out_specs=out_specs, check_vma=False)
```
